32 devices in a mesh: task: 8 (over z, core), tp: 4 (over y, x).
Axes of the slice: x: 2, y: 2, z: 4, core: 2. Of those that a mesh axis runs over, the one named last changes fastest.
Arguments:
- support_x: bfloat16 [8, 384, 3584], P('task'), may hold values from -6 to 6
- adapter_a: bfloat16 [8, 3584, 64], P('task'), may hold values from -0.09375 to 0.09375
- gate_pre: bfloat16 [8, 384, 10240], P('task', None, 'tp'), may hold values from -6 to 6
- lengths: int32 [8], P('task'), may hold values from 128 to 384, as said below
- damping: float32 [8], P('task'), may hold values from 0.03 to 0.3
- down_w: bfloat16 [10240, 3584], P('tp', 'task'), may hold values from -0.0625 to 0.0625
- grad_b: float32 [8, 64, 10240], P('task', None, 'tp'), may hold values from -6 to 6
Outputs:
- solution: float32 [8, 64, 10240], P('task', None, 'tp')
- residual: float32 [8, 64, 10240], P('task', None, 'tp')
The draws below stay inside these ranges and needn't reach their ends.
Inputs may be any that keep to these rules, and one draw needn't show every extreme that they name: `lengths`: each a multiple of 128; some task has exactly 384.
All inputs are finite; a program needn't handle non-finite values.
Results may differ from the reference program's by a relative error of at most 0.033.
Values may be sent and summed in bfloat16 or wider, within the bound.
A program may use at most 64 MiB of HBM per device.

```python
import math
import jax
import jax.numpy as jnp
from jax import lax

D = 3584
FF_WIN = 10240
RANK = 64
BLOCK = 128
LEN = 384
ITERS = 2
TASKS = 8
N_TP = 4


def draw_lengths(key, part):
    blocks = jax.random.randint(key, (TASKS,), 1, LEN // BLOCK + 1)
    chosen = jax.random.randint(jax.random.fold_in(key, 7), (), 0, TASKS)
    blocks = jnp.where(jnp.arange(TASKS) == chosen, LEN // BLOCK, blocks)
    return (blocks * BLOCK).astype(jnp.int32)


def shard_levels(key, extent, split, low, top_value):
    loudness, own = 1.0, jax.random.fold_in(key, 6)
    for dim, shards_of in split:
        draws = jnp.exp(jax.random.uniform(jax.random.fold_in(own, dim), (shards_of,), jnp.float32, low / len(split), top_value / len(split)))
        loudness = loudness * jnp.repeat(draws, extent[dim] // shards_of).reshape([-1 if axis == dim else 1 for axis in range(len(extent))])
    return loudness


def gaussian(rng, shape, scale, reach, pieces=(), kind=jnp.bfloat16):
    values = scale * jax.random.normal(rng, shape, jnp.float32)
    if pieces:
        values = values * shard_levels(rng, shape, pieces, -0.22, 0.18)
    return jnp.clip(values, -reach, reach).astype(kind)


def setup_inputs(seed: int = 0) -> dict:
    streams_of = jax.random.split(jax.random.key(seed), 8)
    support_x = gaussian(streams_of[0], (TASKS, LEN, D), 1.0, 6.0, ((0, 8),))
    adapter_a = gaussian(streams_of[1], (TASKS, D, RANK), D ** -0.5, 0.09375, ((0, 8),))
    gate_pre = gaussian(streams_of[2], (TASKS, LEN, FF_WIN), 1.0, 6.0, ((0, 8), (2, 4)))
    lengths = draw_lengths(jax.random.fold_in(streams_of[7], 71), 0)
    damping = jnp.clip(jnp.exp(math.log(0.3) - 2.3025852 * jax.random.uniform(streams_of[4], (TASKS,), jnp.float32) ** shard_levels(streams_of[4], (TASKS,), ((0, 8),), -0.2, 0.2)), 0.03, 0.3)
    down_w = gaussian(streams_of[5], (FF_WIN, D), FF_WIN ** -0.5, 0.0625, ((0, 4), (1, 8)))
    grad_b = gaussian(streams_of[6], (TASKS, RANK, FF_WIN), 1.0, 6.0, ((0, 8), (2, 4)), jnp.float32)
    return dict(support_x=support_x, adapter_a=adapter_a, gate_pre=gate_pre, lengths=lengths, damping=damping, down_w=down_w, grad_b=grad_b)


def solve_task(operands, down_w):
    support, adapter, gate, length, damping_rate, target = operands
    width = FF_WIN // N_TP
    features = jnp.dot(support, adapter, preferred_element_type=jnp.float32).astype(jnp.bfloat16)
    positions = jnp.arange(LEN, dtype=jnp.int32)[:, None]
    gated = jnp.where(positions < length, jax.nn.silu(gate.astype(jnp.float32)), 0.0).astype(jnp.bfloat16)
    tokens_live = length.astype(jnp.float32)
    weights = down_w.reshape(N_TP, width, D).astype(jnp.float32)

    def apply(vector):
        inner = jnp.dot(features, vector.astype(jnp.bfloat16), preferred_element_type=jnp.float32)
        active = (gated.astype(jnp.float32) * inner).astype(jnp.bfloat16)
        grouped = active.reshape(LEN, N_TP, width).astype(jnp.float32)
        partial_sums = jnp.einsum("lgf,gfd->lgd", grouped, weights)
        rounded = lax.optimization_barrier(partial_sums.astype(jnp.bfloat16))
        mixed = jnp.sum(rounded.astype(jnp.float32), axis=1).astype(jnp.bfloat16)
        back = jnp.dot(mixed, down_w.T, preferred_element_type=jnp.float32)
        second = (gated.astype(jnp.float32) * back).astype(jnp.bfloat16)
        return jnp.dot(features.T, second, preferred_element_type=jnp.float32) / tokens_live + damping_rate * vector

    solution = jnp.zeros_like(target)
    residual = target
    direction = target
    norm_now = jnp.sum(residual * residual)
    for step in range(ITERS):
        image = apply(direction)
        alpha = norm_now / jnp.sum(direction * image)
        solution = solution + alpha * direction
        residual = residual - alpha * image
        norm_next = jnp.sum(residual * residual)
        direction = residual + (norm_next / norm_now) * direction
        norm_now = norm_next
    return solution, residual


def reference(support_x, adapter_a, gate_pre, lengths, damping, down_w, grad_b):
    def per_task(operands):
        return solve_task(operands, down_w)

    return lax.map(per_task, (support_x, adapter_a, gate_pre, lengths, damping, grad_b))
```

```python
import functools

import jax
import jax.numpy as jnp
from jax import lax
from jax.experimental import pallas as pl
from jax.experimental.pallas import tpu as pltpu
from jax.sharding import PartitionSpec as P

ITERS = 2


def shards(support_x, adapter_a, gate_pre, lengths, damping, down_w, grad_b):
    down_full = lax.all_gather(down_w, "task", axis=1, tiled=True)
    features = jnp.dot(support_x[0], adapter_a[0], preferred_element_type=jnp.float32).astype(
        jnp.bfloat16
    )
    positions = lax.broadcasted_iota(jnp.int32, (gate_pre.shape[1], 1), 0)
    gated = jnp.where(
        positions < lengths[0], jax.nn.silu(gate_pre[0].astype(jnp.float32)), 0.0
    ).astype(jnp.bfloat16)
    tokens_live = lengths[0].astype(jnp.float32)
    damping_rate = damping[0]

    def transposed(mixed_rows):
        return lax.dot_general(
            mixed_rows, down_full, (((1,), (1,)), ((), ())), preferred_element_type=jnp.float32
        )

    def apply(vector):
        inner = jnp.dot(features, vector.astype(jnp.bfloat16), preferred_element_type=jnp.float32)
        active = (gated * inner).astype(jnp.bfloat16)
        partial_sum = jnp.dot(active, down_full, preferred_element_type=jnp.float32)
        mixed = lax.psum(partial_sum.astype(jnp.bfloat16), "tp")
        second = (gated * transposed(mixed)).astype(jnp.bfloat16)
        product = lax.dot_general(
            features, second, (((0,), (0,)), ((), ())), preferred_element_type=jnp.float32
        )
        return product / tokens_live + damping_rate * vector

    def paired_sums(vector, image):
        return lax.psum((jnp.sum(vector * vector), jnp.sum(vector * image)), "tp")

    target = grad_b[0]
    solution = jnp.zeros_like(target)
    residual = target
    image = apply(residual)
    norm_now, product = paired_sums(residual, image)
    alpha = norm_now / product
    direction, along = (residual, image)
    for step in range(ITERS):
        solution = solution + alpha * direction
        residual = residual - alpha * along
        if step + 1 < ITERS:
            image = apply(residual)
            norm_next, product = paired_sums(residual, image)
            ratio = norm_next / norm_now
            alpha = norm_next / (product - ratio * norm_next / alpha)
            direction = residual + ratio * direction
            along = image + ratio * along
            norm_now = norm_next
    return (solution[None], residual[None])


MESH = pl.DeviceIdType.MESH


def kernel(
    n_task, n_tp,
    support_hbm, adapter_hbm, gate_hbm, scal_ref, w_hbm, grad_hbm,
    sol_ref, res_ref,
    support, adapter, grad, weights, gated, active, total, features, image0, image1,
    part1, got1, mixed1, part2, got2, mixed2, sums, sums_got,
    load_sem, w_send, d2d_send, w_recv, rs_send1, rs_recv1, ag_send1, ag_recv1,
    rs_send2, rs_recv2, ag_send2, ag_recv2, sum_send, sum_recv,
):
    t_me, j_me = lax.axis_index("task"), lax.axis_index("tp")
    planes = n_task // 2
    z, core = t_me // 2, t_me % 2
    other = 1 - core
    blk = w_hbm.shape[0]
    hidden = w_hbm.shape[1]
    rows = part1.shape[2]
    tile = next(size for size in (512, 256, 128) if hidden % size == 0)
    n_chunk, chunk = part2.shape[0], part2.shape[3]

    def block(t):
        return weights.at[pl.ds(pl.multiple_of(t * blk, 16), blk)]

    own = pltpu.make_async_copy(w_hbm, block(t_me), load_sem.at[0])
    own.start()
    loads = [
        pltpu.make_async_copy(source, target, load_sem.at[1 + place])
        for place, (source, target) in enumerate(
            ((gate_hbm, active), (support_hbm, support), (adapter_hbm, adapter), (grad_hbm, grad))
        )
    ]
    for load in loads:
        load.start()

    up, down = {"task": t_me + 2, "tp": j_me}, {"task": t_me - 2, "tp": j_me}
    partner = {"task": 2 * z + other, "tp": j_me}
    peers = [{"task": t_me, "tp": lax.rem(j_me + d, n_tp)} for d in range(1, n_tp)]

    barrier = pltpu.get_barrier_semaphore()
    for peer in [partner] + peers:
        pl.semaphore_signal(barrier, inc=1, device_id=peer, device_id_type=MESH)

    @pl.when(z < planes - 1)
    def _():
        pl.semaphore_signal(barrier, inc=1, device_id=up, device_id_type=MESH)

    @pl.when(z > 0)
    def _():
        pl.semaphore_signal(barrier, inc=1, device_id=down, device_id_type=MESH)

    pl.semaphore_wait(barrier, n_tp + lax.min(z, 1) + lax.min(planes - 1 - z, 1))
    own.wait()

    def send_block(t, target, send_sem):
        return pltpu.make_async_remote_copy(
            src_ref=block(t), dst_ref=block(t), send_sem=send_sem, recv_sem=w_recv.at[t],
            device_id=target, device_id_type=MESH,
        )

    def arrived(t):
        pltpu.make_async_copy(block(t), block(t), w_recv.at[t]).wait()

    def pass_on(plane, d, from_left):
        t = 2 * plane + core

        @pl.when(d > 0)
        def _():
            arrived(t)

        if from_left:
            @pl.when(z < planes - 1)
            def _():
                send_block(t, up, w_send.at[0, t]).start()

        @pl.when((z > 0) & ((d == 0) | (not from_left)))
        def _():
            send_block(t, down, w_send.at[1, t]).start()

        send_block(t, partner, d2d_send.at[t]).start()

    pass_on(z, 0, True)

    loads[1].wait()
    loads[2].wait()
    features[...] = jnp.dot(
        support[...], adapter[...], preferred_element_type=jnp.float32
    ).astype(jnp.bfloat16)
    loads[0].wait()
    live, rate = scal_ref[0:1, 0:1], scal_ref[1:2, 0:1]
    tokens = active.shape[0]
    positions = lax.broadcasted_iota(jnp.int32, (tokens, tile), 0).astype(jnp.float32)

    def columns(i):
        return pl.ds(pl.multiple_of(i * tile, tile), tile)

    @pl.loop(0, hidden // tile)
    def _(i):
        pre = active[:, columns(i)].astype(jnp.float32)
        gated[:, columns(i)] = jnp.where(
            positions < live, pre / (1.0 + jnp.exp(-pre)), 0.0
        ).astype(jnp.bfloat16)

    loads[3].wait()

    def make_active(vector):
        @pl.loop(0, hidden // tile)
        def _(i):
            inner = jnp.dot(
                features[...], vector[:, columns(i)].astype(jnp.bfloat16),
                preferred_element_type=jnp.float32,
            )
            active[:, columns(i)] = (gated[:, columns(i)].astype(jnp.float32) * inner).astype(
                jnp.bfloat16
            )
            total[:, columns(i)] = jnp.zeros_like(inner)

    def product(which, first, size, part, got, send_sem, recv_sem):
        span = pl.ds(pl.multiple_of(first, 16), size)
        partial_sum = lax.dot_general(
            active[...], weights[span, :], (((1,), (1,)), ((), ())),
            preferred_element_type=jnp.float32,
        )
        part[which] = partial_sum.astype(jnp.bfloat16).reshape(n_tp, rows, size)
        for d in range(1, n_tp):
            pltpu.make_async_remote_copy(
                src_ref=part.at[which, lax.rem(j_me + d, n_tp)], dst_ref=got.at[which, d - 1],
                send_sem=send_sem.at[which], recv_sem=recv_sem.at[which],
                device_id=peers[d - 1], device_id_type=MESH,
            ).start()

    def reduce(which, part, got, mixed, recv_sem, send_sem, out_sem):
        pltpu.make_async_copy(got.at[which], got.at[which], recv_sem.at[which]).wait()
        added = part[which, j_me].astype(jnp.float32)
        for d in range(1, n_tp):
            added = added + got[which, d - 1].astype(jnp.float32)
        mixed[which, j_me] = added.astype(jnp.bfloat16)
        for d in range(1, n_tp):
            pltpu.make_async_remote_copy(
                src_ref=mixed.at[which, j_me], dst_ref=mixed.at[which, j_me],
                send_sem=send_sem.at[which], recv_sem=out_sem.at[which],
                device_id=peers[d - 1], device_id_type=MESH,
            ).start()

    def back(which, first, size, mixed, out_sem):
        pieces = mixed.at[which, pl.ds(0, n_tp - 1)]
        pltpu.make_async_copy(pieces, pieces, out_sem.at[which]).wait()
        span = pl.ds(pl.multiple_of(first, 16), size)
        whole = mixed[which].reshape(n_tp * rows, size)

        @pl.loop(0, hidden // tile)
        def _(i):
            total[:, columns(i)] += jnp.dot(
                whole, weights[span, columns(i)], preferred_element_type=jnp.float32
            )

    def make_image(vector, image, slot):
        def body(i, carry):
            second = (gated[:, columns(i)].astype(jnp.float32) * total[:, columns(i)]).astype(
                jnp.bfloat16
            )
            outer = lax.dot_general(
                features[...], second, (((0,), (0,)), ((), ())),
                preferred_element_type=jnp.float32,
            )
            v = vector[:, columns(i)]
            value = outer / live + rate * v
            image[:, columns(i)] = value
            return carry[0] + v * v, carry[1] + v * value

        zero = jnp.zeros((vector.shape[0], tile), jnp.float32)
        squares, crosses = lax.fori_loop(0, hidden // tile, body, (zero, zero))
        sums[slot, 0] = jnp.broadcast_to(jnp.sum(squares, keepdims=True), (8, 128))
        sums[slot, 1] = jnp.broadcast_to(jnp.sum(crosses, keepdims=True), (8, 128))
        for d in range(1, n_tp):
            pltpu.make_async_remote_copy(
                src_ref=sums.at[slot], dst_ref=sums_got.at[slot, d - 1],
                send_sem=sum_send.at[slot], recv_sem=sum_recv.at[slot],
                device_id=peers[d - 1], device_id_type=MESH,
            ).start()
        got = sums_got.at[slot]
        pltpu.make_async_copy(got, got, sum_recv.at[slot]).wait()
        norm, cross = sums[slot, 0, 0:1, 0:1], sums[slot, 1, 0:1, 0:1]
        for d in range(1, n_tp):
            norm = norm + sums_got[slot, d - 1, 0, 0:1, 0:1]
            cross = cross + sums_got[slot, d - 1, 1, 0:1, 0:1]
        return norm, cross

    make_active(grad)

    @pl.loop(0, planes)
    def _(d):
        left, right = z - d, z + d

        @pl.when((d > 0) & (left >= 0))
        def _():
            pass_on(left, d, True)

        @pl.when((d > 0) & (right < planes))
        def _():
            pass_on(right, d, False)

        for stage in range(3):
            for plane, there in ((left, left >= 0), (right, (d > 0) & (right < planes))):
                for side in (core, other):
                    @pl.when(there)
                    def _(plane=plane, side=side, mine=side is core, stage=stage):
                        t = 2 * plane + side
                        if stage == 0:
                            if not mine:
                                arrived(t)
                            product(t, t * blk, blk, part1, got1, rs_send1, rs_recv1)
                        elif stage == 1:
                            reduce(t, part1, got1, mixed1, rs_recv1, ag_send1, ag_recv1)
                        else:
                            back(t, t * blk, blk, mixed1, ag_recv1)

    norm0, cross0 = make_image(grad, image0, 0)
    alpha0 = norm0 / cross0

    @pl.loop(0, hidden // tile)
    def _(i):
        res_ref[:, columns(i)] = grad[:, columns(i)] - alpha0 * image0[:, columns(i)]

    make_active(res_ref)

    @pl.loop(0, n_chunk)
    def _(k):
        product(k, k * chunk, chunk, part2, got2, rs_send2, rs_recv2)

    @pl.loop(0, n_chunk)
    def _(k):
        reduce(k, part2, got2, mixed2, rs_recv2, ag_send2, ag_recv2)

    @pl.loop(0, n_chunk)
    def _(k):
        back(k, k * chunk, chunk, mixed2, ag_recv2)

    norm1, cross1 = make_image(res_ref, image1, 1)
    ratio = norm1 / norm0
    alpha1 = norm1 / (cross1 - ratio * norm1 / alpha0)

    @pl.loop(0, hidden // tile)
    def _(i):
        first, then = grad[:, columns(i)], res_ref[:, columns(i)]
        sol_ref[:, columns(i)] = alpha0 * first + alpha1 * (then + ratio * first)
        res_ref[:, columns(i)] = then - alpha1 * (
            image1[:, columns(i)] + ratio * image0[:, columns(i)]
        )

    def drained(ref, sem):
        pltpu.make_async_copy(ref, ref, sem).wait()

    @pl.loop(0, n_task)
    def _(t):
        @pl.when((t % 2 == core) & (t // 2 <= z) & (z < planes - 1))
        def _():
            drained(block(t), w_send.at[0, t])

        @pl.when((t % 2 == core) & (t // 2 >= z) & (z > 0))
        def _():
            drained(block(t), w_send.at[1, t])

        @pl.when(t % 2 == core)
        def _():
            drained(block(t), d2d_send.at[t])

        drained(got1.at[t], rs_send1.at[t])
        drained(got1.at[t], ag_send1.at[t])

    @pl.loop(0, n_chunk)
    def _(k):
        drained(got2.at[k], rs_send2.at[k])
        drained(got2.at[k], ag_send2.at[k])

    for slot in range(2):
        drained(sums_got.at[slot], sum_send.at[slot])


def fused(n_task, n_tp, support_x, adapter_a, gate_pre, lengths, damping, down_w, grad_b):
    tokens, width = support_x.shape[1:]
    rank = adapter_a.shape[2]
    hidden, blk = down_w.shape
    rows = tokens // n_tp
    chunk = next(size for size in (512, 256, 128) if width % size == 0)
    n_chunk = width // chunk
    scal = jnp.broadcast_to(
        jnp.concatenate([lengths.astype(jnp.float32), damping])[:, None], (2, 128)
    )
    f32, bf16 = jnp.float32, jnp.bfloat16
    dma = pltpu.SemaphoreType.DMA
    anywhere, vmem = pl.BlockSpec(memory_space=pl.ANY), pl.BlockSpec(memory_space=pltpu.VMEM)
    shape = jax.ShapeDtypeStruct((rank, hidden), f32)
    solved, residual = pl.pallas_call(
        functools.partial(kernel, n_task, n_tp),
        out_shape=(shape, shape),
        in_specs=[anywhere, anywhere, anywhere, vmem, anywhere, anywhere],
        out_specs=(vmem, vmem),
        scratch_shapes=[
            pltpu.VMEM((tokens, width), bf16),
            pltpu.VMEM((width, rank), bf16),
            pltpu.VMEM((rank, hidden), f32),
            pltpu.VMEM((width, hidden), bf16),
            pltpu.VMEM((tokens, hidden), bf16),
            pltpu.VMEM((tokens, hidden), bf16),
            pltpu.VMEM((tokens, hidden), f32),
            pltpu.VMEM((tokens, rank), bf16),
            pltpu.VMEM((rank, hidden), f32),
            pltpu.VMEM((rank, hidden), f32),
            pltpu.VMEM((n_task, n_tp, rows, blk), bf16),
            pltpu.VMEM((n_task, n_tp - 1, rows, blk), bf16),
            pltpu.VMEM((n_task, n_tp, rows, blk), bf16),
            pltpu.VMEM((n_chunk, n_tp, rows, chunk), bf16),
            pltpu.VMEM((n_chunk, n_tp - 1, rows, chunk), bf16),
            pltpu.VMEM((n_chunk, n_tp, rows, chunk), bf16),
            pltpu.VMEM((2, 2, 8, 128), f32),
            pltpu.VMEM((2, n_tp - 1, 2, 8, 128), f32),
            dma((5,)),
            dma((2, n_task)),
            dma((n_task,)),
            dma((n_task,)),
            dma((n_task,)),
            dma((n_task,)),
            dma((n_task,)),
            dma((n_task,)),
            dma((n_chunk,)),
            dma((n_chunk,)),
            dma((n_chunk,)),
            dma((n_chunk,)),
            dma((2,)),
            dma((2,)),
        ],
        compiler_params=pltpu.CompilerParams(
            collective_id=0, has_side_effects=True, vmem_limit_bytes=66_000_000
        ),
    )(support_x[0], adapter_a[0], gate_pre[0], scal, down_w.T, grad_b[0])
    return solved[None], residual[None]


def solution(mesh):
    in_specs = (
        P("task", None, None),
        P("task", None, None),
        P("task", None, "tp"),
        P("task"),
        P("task"),
        P("tp", "task"),
        P("task", None, "tp"),
    )
    out_specs = (P("task", None, "tp"), P("task", None, "tp"))
    n_task, n_tp = mesh.shape["task"], mesh.shape["tp"]

    def body(support_x, *rest):
        if support_x.shape[1] % (16 * n_tp):
            return shards(support_x, *rest)
        return fused(n_task, n_tp, support_x, *rest)

    return jax.shard_map(body, mesh=mesh, in_specs=in_specs, out_specs=out_specs, check_vma=False)
```

```python
import functools

import jax
import jax.numpy as jnp
from jax import lax
from jax.experimental import pallas as pl
from jax.experimental.pallas import tpu as pltpu
from jax.sharding import PartitionSpec as P

ITERS = 2


def shards(support_x, adapter_a, gate_pre, lengths, damping, down_w, grad_b):
    down_full = lax.all_gather(down_w, "task", axis=1, tiled=True)
    features = jnp.dot(support_x[0], adapter_a[0], preferred_element_type=jnp.float32).astype(
        jnp.bfloat16
    )
    positions = lax.broadcasted_iota(jnp.int32, (gate_pre.shape[1], 1), 0)
    gated = jnp.where(
        positions < lengths[0], jax.nn.silu(gate_pre[0].astype(jnp.float32)), 0.0
    ).astype(jnp.bfloat16)
    tokens_live = lengths[0].astype(jnp.float32)
    damping_rate = damping[0]

    def transposed(mixed_rows):
        return lax.dot_general(
            mixed_rows, down_full, (((1,), (1,)), ((), ())), preferred_element_type=jnp.float32
        )

    def apply(vector):
        inner = jnp.dot(features, vector.astype(jnp.bfloat16), preferred_element_type=jnp.float32)
        active = (gated * inner).astype(jnp.bfloat16)
        partial_sum = jnp.dot(active, down_full, preferred_element_type=jnp.float32)
        mixed = lax.psum(partial_sum.astype(jnp.bfloat16), "tp")
        second = (gated * transposed(mixed)).astype(jnp.bfloat16)
        product = lax.dot_general(
            features, second, (((0,), (0,)), ((), ())), preferred_element_type=jnp.float32
        )
        return product / tokens_live + damping_rate * vector

    def paired_sums(vector, image):
        return lax.psum((jnp.sum(vector * vector), jnp.sum(vector * image)), "tp")

    target = grad_b[0]
    solution = jnp.zeros_like(target)
    residual = target
    image = apply(residual)
    norm_now, product = paired_sums(residual, image)
    alpha = norm_now / product
    direction, along = (residual, image)
    for step in range(ITERS):
        solution = solution + alpha * direction
        residual = residual - alpha * along
        if step + 1 < ITERS:
            image = apply(residual)
            norm_next, product = paired_sums(residual, image)
            ratio = norm_next / norm_now
            alpha = norm_next / (product - ratio * norm_next / alpha)
            direction = residual + ratio * direction
            along = image + ratio * along
            norm_now = norm_next
    return (solution[None], residual[None])


MESH = pl.DeviceIdType.MESH


def kernel(
    n_task, n_tp,
    support_hbm, adapter_hbm, gate_hbm, scal_ref, w_hbm, grad_hbm,
    sol_ref, res_ref,
    support, adapter, grad, weights, gated, active, total, features, image0, image1,
    part1, got1, mixed1, part2, got2, mixed2, sums, sums_got,
    load_sem, w_send, d2d_send, w_recv, rs_send1, rs_recv1, ag_send1, ag_recv1,
    rs_send2, rs_recv2, ag_send2, ag_recv2, fw_send, fw_recv, sum_send, sum_recv,
):
    t_me, j_me = lax.axis_index("task"), lax.axis_index("tp")
    planes = n_task // 2
    z, core = t_me // 2, t_me % 2
    other = 1 - core
    blk = part1.shape[3]
    subs = w_hbm.shape[0] // blk
    hidden = w_hbm.shape[1]
    rows = part1.shape[2]
    tile = next(size for size in (512, 256, 128) if hidden % size == 0)
    n_chunk, chunk = part2.shape[0], part2.shape[3]

    def block(u):
        return weights.at[pl.ds(pl.multiple_of(u * blk, 16), blk)]

    mine_all = weights.at[pl.ds(pl.multiple_of(t_me * subs * blk, 16), subs * blk)]
    own = pltpu.make_async_copy(w_hbm, mine_all, load_sem.at[0])
    own.start()
    loads = [
        pltpu.make_async_copy(source, target, load_sem.at[1 + place])
        for place, (source, target) in enumerate(
            ((gate_hbm, active), (support_hbm, support), (adapter_hbm, adapter), (grad_hbm, grad))
        )
    ]
    for load in loads:
        load.start()

    up, down = {"task": t_me + 2, "tp": j_me}, {"task": t_me - 2, "tp": j_me}
    partner = {"task": 2 * z + other, "tp": j_me}
    peers = [{"task": t_me, "tp": lax.rem(j_me + d, n_tp)} for d in range(1, n_tp)]

    barrier = pltpu.get_barrier_semaphore()
    for peer in [partner] + peers:
        pl.semaphore_signal(barrier, inc=1, device_id=peer, device_id_type=MESH)

    @pl.when(z < planes - 1)
    def _():
        pl.semaphore_signal(barrier, inc=1, device_id=up, device_id_type=MESH)

    @pl.when(z > 0)
    def _():
        pl.semaphore_signal(barrier, inc=1, device_id=down, device_id_type=MESH)

    pl.semaphore_wait(barrier, n_tp + lax.min(z, 1) + lax.min(planes - 1 - z, 1))
    own.wait()

    def send_block(t, target, send_sem):
        return pltpu.make_async_remote_copy(
            src_ref=block(t), dst_ref=block(t), send_sem=send_sem, recv_sem=w_recv.at[t],
            device_id=target, device_id_type=MESH,
        )

    def arrived(t):
        pltpu.make_async_copy(block(t), block(t), w_recv.at[t]).wait()

    def pass_on(plane, s, d, from_left):
        t = (2 * plane + core) * subs + s

        @pl.when(d > 0)
        def _():
            arrived(t)

        if from_left:
            @pl.when(z < planes - 1)
            def _():
                send_block(t, up, w_send.at[0, t]).start()

        @pl.when((z > 0) & ((d == 0) | (not from_left)))
        def _():
            send_block(t, down, w_send.at[1, t]).start()

        send_block(t, partner, d2d_send.at[t]).start()

    for s in range(subs):
        pass_on(z, s, 0, True)

    loads[1].wait()
    loads[2].wait()
    features[...] = jnp.dot(
        support[...], adapter[...], preferred_element_type=jnp.float32
    ).astype(jnp.bfloat16)
    loads[0].wait()
    live, rate = scal_ref[0:1, 0:1], scal_ref[1:2, 0:1]
    tokens = active.shape[0]
    positions = lax.broadcasted_iota(jnp.int32, (tokens, tile), 0).astype(jnp.float32)

    def columns(i):
        return pl.ds(pl.multiple_of(i * tile, tile), tile)

    @pl.loop(0, hidden // tile)
    def _(i):
        pre = active[:, columns(i)].astype(jnp.float32)
        gated[:, columns(i)] = jnp.where(
            positions < live, pre / (1.0 + jnp.exp(-pre)), 0.0
        ).astype(jnp.bfloat16)

    loads[3].wait()

    def make_active(vector):
        @pl.loop(0, hidden // tile)
        def _(i):
            inner = jnp.dot(
                features[...], vector[:, columns(i)].astype(jnp.bfloat16),
                preferred_element_type=jnp.float32,
            )
            active[:, columns(i)] = (gated[:, columns(i)].astype(jnp.float32) * inner).astype(
                jnp.bfloat16
            )
            total[:, columns(i)] = jnp.zeros_like(inner)

    def product(which, first, size, part, got, send_sem, recv_sem):
        span = pl.ds(pl.multiple_of(first, 16), size)
        partial_sum = lax.dot_general(
            active[...], weights[span, :], (((1,), (1,)), ((), ())),
            preferred_element_type=jnp.float32,
        )
        part[which] = partial_sum.astype(jnp.bfloat16).reshape(n_tp, rows, size)
        for d in range(1, n_tp):
            pltpu.make_async_remote_copy(
                src_ref=part.at[which, lax.rem(j_me + d, n_tp)], dst_ref=got.at[which, d - 1],
                send_sem=send_sem.at[which], recv_sem=recv_sem.at[which],
                device_id=peers[d - 1], device_id_type=MESH,
            ).start()

    def reduce(which, part, got, mixed, recv_sem, send_sem, out_sem, targets):
        pltpu.make_async_copy(got.at[which], got.at[which], recv_sem.at[which]).wait()
        added = part[which, j_me].astype(jnp.float32)
        for d in range(1, n_tp):
            added = added + got[which, d - 1].astype(jnp.float32)
        mixed[which, j_me] = added.astype(jnp.bfloat16)
        for target in targets:
            pltpu.make_async_remote_copy(
                src_ref=mixed.at[which, j_me], dst_ref=mixed.at[which, j_me],
                send_sem=send_sem.at[which], recv_sem=out_sem.at[which],
                device_id=target, device_id_type=MESH,
            ).start()

    def back(which, first, size, mixed):
        span = pl.ds(pl.multiple_of(first, 16), size)
        whole = mixed[which].reshape(n_tp * rows, size)

        @pl.loop(0, hidden // tile)
        def _(i):
            total[:, columns(i)] += jnp.dot(
                whole, weights[span, columns(i)], preferred_element_type=jnp.float32
            )

    def make_image(vector, image, slot):
        def body(i, carry):
            second = (gated[:, columns(i)].astype(jnp.float32) * total[:, columns(i)]).astype(
                jnp.bfloat16
            )
            outer = lax.dot_general(
                features[...], second, (((0,), (0,)), ((), ())),
                preferred_element_type=jnp.float32,
            )
            v = vector[:, columns(i)]
            value = outer / live + rate * v
            image[:, columns(i)] = value
            return carry[0] + v * v, carry[1] + v * value

        zero = jnp.zeros((vector.shape[0], tile), jnp.float32)
        squares, crosses = lax.fori_loop(0, hidden // tile, body, (zero, zero))
        sums[slot, 0] = jnp.broadcast_to(jnp.sum(squares, keepdims=True), (8, 128))
        sums[slot, 1] = jnp.broadcast_to(jnp.sum(crosses, keepdims=True), (8, 128))
        for d in range(1, n_tp):
            pltpu.make_async_remote_copy(
                src_ref=sums.at[slot], dst_ref=sums_got.at[slot, d - 1],
                send_sem=sum_send.at[slot], recv_sem=sum_recv.at[slot],
                device_id=peers[d - 1], device_id_type=MESH,
            ).start()
        got = sums_got.at[slot]
        pltpu.make_async_copy(got, got, sum_recv.at[slot]).wait()
        norm, cross = sums[slot, 0, 0:1, 0:1], sums[slot, 1, 0:1, 0:1]
        for d in range(1, n_tp):
            norm = norm + sums_got[slot, d - 1, 0, 0:1, 0:1]
            cross = cross + sums_got[slot, d - 1, 1, 0:1, 0:1]
        return norm, cross

    make_active(grad)

    @pl.loop(0, planes * subs)
    def _(e):
        d, s = e // subs, e % subs
        left, right = z - d, z + d

        @pl.when((d > 0) & (left >= 0))
        def _():
            pass_on(left, s, d, True)

        @pl.when((d > 0) & (right < planes))
        def _():
            pass_on(right, s, d, False)

        for stage in range(3):
            for plane, there in ((left, left >= 0), (right, (d > 0) & (right < planes))):
                for side in (core, other):
                    @pl.when(there)
                    def _(plane=plane, side=side, mine=side is core, stage=stage):
                        t = (2 * plane + side) * subs + s
                        if stage == 0:
                            if not mine:
                                arrived(t)
                            product(t, t * blk, blk, part1, got1, rs_send1, rs_recv1)
                        elif stage == 1:
                            reduce(t, part1, got1, mixed1, rs_recv1, ag_send1, ag_recv1, peers)
                        else:
                            pieces = mixed1.at[t, pl.ds(0, n_tp - 1)]
                            pltpu.make_async_copy(pieces, pieces, ag_recv1.at[t]).wait()
                            back(t, t * blk, blk, mixed1)

    norm0, cross0 = make_image(grad, image0, 0)
    alpha0 = norm0 / cross0

    @pl.loop(0, hidden // tile)
    def _(i):
        res_ref[:, columns(i)] = grad[:, columns(i)] - alpha0 * image0[:, columns(i)]

    make_active(res_ref)

    @pl.loop(0, n_chunk)
    def _(k):
        product(k, k * chunk, chunk, part2, got2, rs_send2, rs_recv2)

    row, col = j_me // 2, j_me % 2
    beside, below = 2 * row + 1 - col, 2 * (1 - row) + col
    half = rows // 2
    near = [{"task": t_me, "tp": beside}, {"task": t_me, "tp": below}]

    @pl.loop(0, n_chunk)
    def _(k):
        reduce(k, part2, got2, mixed2, rs_recv2, ag_send2, ag_recv2, near)

    def finish(k):
        piece = mixed2.at[k, 0]
        pltpu.make_async_copy(piece, piece, fw_recv.at[k]).wait()
        back(k, k * chunk, chunk, mixed2)

    @pl.loop(0, n_chunk)
    def _(k):
        pieces = mixed2.at[k, pl.ds(0, 2)]
        pltpu.make_async_copy(pieces, pieces, ag_recv2.at[k]).wait()
        for source, start, target in ((beside, 0, near[1]), (below, half, near[0])):
            piece = mixed2.at[k, source, pl.ds(start, half)]
            pltpu.make_async_remote_copy(
                src_ref=piece, dst_ref=piece, send_sem=fw_send.at[k], recv_sem=fw_recv.at[k],
                device_id=target, device_id_type=MESH,
            ).start()

        @pl.when(k > 0)
        def _():
            finish(k - 1)

    finish(n_chunk - 1)

    norm1, cross1 = make_image(res_ref, image1, 1)
    ratio = norm1 / norm0
    alpha1 = norm1 / (cross1 - ratio * norm1 / alpha0)

    @pl.loop(0, hidden // tile)
    def _(i):
        first, then = grad[:, columns(i)], res_ref[:, columns(i)]
        sol_ref[:, columns(i)] = alpha0 * first + alpha1 * (then + ratio * first)
        res_ref[:, columns(i)] = then - alpha1 * (
            image1[:, columns(i)] + ratio * image0[:, columns(i)]
        )

    def drained(ref, sem):
        pltpu.make_async_copy(ref, ref, sem).wait()

    @pl.loop(0, n_task * subs)
    def _(t):
        task = t // subs

        @pl.when((task % 2 == core) & (task // 2 <= z) & (z < planes - 1))
        def _():
            drained(block(t), w_send.at[0, t])

        @pl.when((task % 2 == core) & (task // 2 >= z) & (z > 0))
        def _():
            drained(block(t), w_send.at[1, t])

        @pl.when(task % 2 == core)
        def _():
            drained(block(t), d2d_send.at[t])

        drained(got1.at[t], rs_send1.at[t])
        drained(got1.at[t], ag_send1.at[t])

    @pl.loop(0, n_chunk)
    def _(k):
        drained(got2.at[k], rs_send2.at[k])
        drained(mixed2.at[k, pl.ds(0, 2)], ag_send2.at[k])
        drained(mixed2.at[k, 0], fw_send.at[k])

    for slot in range(2):
        drained(sums_got.at[slot], sum_send.at[slot])


def fused(n_task, n_tp, support_x, adapter_a, gate_pre, lengths, damping, down_w, grad_b):
    tokens, width = support_x.shape[1:]
    rank = adapter_a.shape[2]
    hidden, share = down_w.shape
    blk = share // 2 if share % 32 == 0 else share
    n_block = n_task * share // blk
    rows = tokens // n_tp
    chunk = next(size for size in (512, 256, 128) if width % size == 0)
    n_chunk = width // chunk
    scal = jnp.broadcast_to(
        jnp.concatenate([lengths.astype(jnp.float32), damping])[:, None], (2, 128)
    )
    f32, bf16 = jnp.float32, jnp.bfloat16
    dma = pltpu.SemaphoreType.DMA
    anywhere, vmem = pl.BlockSpec(memory_space=pl.ANY), pl.BlockSpec(memory_space=pltpu.VMEM)
    shape = jax.ShapeDtypeStruct((rank, hidden), f32)
    solved, residual = pl.pallas_call(
        functools.partial(kernel, n_task, n_tp),
        out_shape=(shape, shape),
        in_specs=[anywhere, anywhere, anywhere, vmem, anywhere, anywhere],
        out_specs=(vmem, vmem),
        scratch_shapes=[
            pltpu.VMEM((tokens, width), bf16),
            pltpu.VMEM((width, rank), bf16),
            pltpu.VMEM((rank, hidden), f32),
            pltpu.VMEM((width, hidden), bf16),
            pltpu.VMEM((tokens, hidden), bf16),
            pltpu.VMEM((tokens, hidden), bf16),
            pltpu.VMEM((tokens, hidden), f32),
            pltpu.VMEM((tokens, rank), bf16),
            pltpu.VMEM((rank, hidden), f32),
            pltpu.VMEM((rank, hidden), f32),
            pltpu.VMEM((n_block, n_tp, rows, blk), bf16),
            pltpu.VMEM((n_block, n_tp - 1, rows, blk), bf16),
            pltpu.VMEM((n_block, n_tp, rows, blk), bf16),
            pltpu.VMEM((n_chunk, n_tp, rows, chunk), bf16),
            pltpu.VMEM((n_chunk, n_tp - 1, rows, chunk), bf16),
            pltpu.VMEM((n_chunk, n_tp, rows, chunk), bf16),
            pltpu.VMEM((2, 2, 8, 128), f32),
            pltpu.VMEM((2, n_tp - 1, 2, 8, 128), f32),
            dma((5,)),
            dma((2, n_block)),
            dma((n_block,)),
            dma((n_block,)),
            dma((n_block,)),
            dma((n_block,)),
            dma((n_block,)),
            dma((n_block,)),
            dma((n_chunk,)),
            dma((n_chunk,)),
            dma((n_chunk,)),
            dma((n_chunk,)),
            dma((n_chunk,)),
            dma((n_chunk,)),
            dma((2,)),
            dma((2,)),
        ],
        compiler_params=pltpu.CompilerParams(
            collective_id=0, has_side_effects=True, vmem_limit_bytes=66_000_000
        ),
    )(support_x[0], adapter_a[0], gate_pre[0], scal, down_w.T, grad_b[0])
    return solved[None], residual[None]


def solution(mesh):
    in_specs = (
        P("task", None, None),
        P("task", None, None),
        P("task", None, "tp"),
        P("task"),
        P("task"),
        P("tp", "task"),
        P("task", None, "tp"),
    )
    out_specs = (P("task", None, "tp"), P("task", None, "tp"))
    n_task, n_tp = mesh.shape["task"], mesh.shape["tp"]

    def body(support_x, *rest):
        if n_tp != 4 or support_x.shape[1] % (32 * n_tp):
            return shards(support_x, *rest)
        return fused(n_task, n_tp, support_x, *rest)

    return jax.shard_map(body, mesh=mesh, in_specs=in_specs, out_specs=out_specs, check_vma=False)
```
